32 devices in a mesh: dp: 8 (over z, y), expert: 4 (over x, core).
Axes of the slice: x: 2, y: 2, z: 4, core: 2. Of those that a mesh axis runs over, the one named last changes fastest.
Arguments:
- tokens: bfloat16 [1024, 4096], P('dp'), may hold values from -6 to 6
- expert_ids: int32 [1024, 2], P('dp'), may hold values from 0 to 3, all different within a row; in each aligned block of 128 rows (0 to 127, 128 to 255, ...) at most 96 rows name the same one
- gate_weights: float32 [1024, 2], P('dp'), may hold values from 0.2 to 1
- live_counts: int32 [8], P('dp'), may hold values from 64 to 128, as said below
- w_gate: bfloat16 [4, 4096, 8192], P('expert', None, 'dp'), may hold values from -0.09375 to 0.09375
- w_up: bfloat16 [4, 4096, 8192], P('expert', None, 'dp'), may hold values from -0.09375 to 0.09375
- w_down: bfloat16 [4, 8192, 4096], P('expert', 'dp'), may hold values from -0.0625 to 0.0625
Outputs:
- mixed: bfloat16 [1024, 4096], P('dp')
- total_loads: int32 [4], replicated
The draws below stay inside these ranges and needn't reach their ends.
Inputs may be any that keep to these rules, and one draw needn't show every extreme that they name: `expert_ids`: each token names two different experts. Among the tokens of one rank no expert is named more than 96 times, a bound that some block reaches in some ranks. Rank r's first live_counts[r] tokens are live, the rest are padding. Some rank has all 128 tokens live.
All inputs are finite; a program needn't handle non-finite values.
Results may differ from the reference program's by a relative error of at most 0.017.
Values may be sent and summed in bfloat16 or wider, within the bound.
A program may use at most 128 MiB of HBM per device.

```python
import math
import jax
import jax.numpy as jnp
import numpy as np
from jax import lax

D = 4096
FF = 8192
TOK_DEV = 128
EXPERTS = 4
CAP = 96
RANKS = 8
TOKENS = 1024
N_DP = 8


def draw_live_counts(key, part):
    base = jax.random.fold_in(key, 11)
    first_key, second_key = jax.random.split(base)
    counts = jax.random.randint(first_key, (RANKS,), TOK_DEV // 2, TOK_DEV + 1)
    full_rank = jax.random.randint(second_key, (), 0, RANKS)
    return jnp.where(jnp.arange(RANKS) == full_rank, TOK_DEV, counts).astype(jnp.int32)


def shard_levels(rng, dims, cuts, smallest, high):
    loudness = 1.0
    for axis_at, blocks in cuts:
        draws = jax.random.uniform(jax.random.fold_in(jax.random.fold_in(rng, 6), axis_at), (blocks,), jnp.float32, smallest / len(cuts), high / len(cuts))
        loudness = loudness * jnp.repeat(jnp.exp(draws), dims[axis_at] // blocks).reshape((-1,) + (1,) * (len(dims) - 1 - axis_at))
    return loudness


def shared_out(rng, own, number, rows, count, top, bound, slope):
    ranking = jax.random.permutation(rng, count)
    packed, usual = load_shares(count, rows * top, bound, slope, True), load_shares(count, rows * top, bound, slope, False)
    places = jnp.arange(count)

    def named(sizes, offset_by):
        used = int((sizes > 0).sum())
        fixed = max(1, used // 4)
        passed = fixed + (places - fixed + offset_by * (used - fixed)) % max(1, count - fixed)
        return jnp.zeros((count,), jnp.int32).at[ranking[jnp.where(places < fixed, places, passed)]].set(jnp.asarray(sizes, jnp.int32))

    sizes = jnp.where(number % 4 == 0, named(packed, number // 4), named(usual, number - number // 4 - 1))
    mixed = jax.random.permutation(jax.random.fold_in(own, 3), count)
    donor, receiver = mixed[0:count // 2 * 2:2], mixed[1:count // 2 * 2:2]
    margin = jnp.minimum(sizes[donor] - 1, bound - sizes[receiver]) // 2
    margin = jnp.where((donor == ranking[0]) | (receiver == ranking[0]) | (sizes[receiver] == 0), 0, jnp.maximum(margin, 0))
    passed = jax.random.randint(jax.random.fold_in(own, 4), (count // 2,), 0, 1 << 20) % (margin + 1)
    sizes = sizes.at[donor].add(-passed).at[receiver].add(passed)
    items = jnp.searchsorted(jnp.cumsum(sizes), jnp.arange(rows * top), side="right").astype(jnp.int32)
    grid = items.reshape(top, rows).T
    grid = grid[jax.random.permutation(jax.random.fold_in(own, 1), rows)]
    offset_by = jax.random.randint(jax.random.fold_in(own, 2), (rows, 1), 0, top)
    return jnp.take_along_axis(grid, (jnp.arange(top)[None, :] + offset_by) % top, axis=1)


def load_shares(amount, total, bound, lean, full):
    portions = [(1 << 20) // math.isqrt(standing ** lean) + 1 for standing in range(1, amount + 1)]
    largest = bound if full else min(bound, max(-(-total // amount), total * portions[0] // sum(portions)))
    least = 1 if total - largest >= amount - 1 else 0
    given, spare = [largest] + [least] * (amount - 1), total - largest - least * (amount - 1)
    while spare > 0:
        movable = [i for i in range(1, amount) if given[i] < largest] or [i for i in range(1, amount) if given[i] < bound]
        whole, left = sum([portions[i] for i in movable]), spare
        for i in movable:
            more = min(bound - given[i], max(1, left * portions[i] // whole), spare)
            given[i] = given[i] + more
            spare = spare - more
    return np.array(given)


def gaussian(own_key, extent, width, bound, pieces=(), held_as=jnp.bfloat16):
    result = width * jax.random.normal(own_key, extent, jnp.float32)
    if pieces:
        result = result * shard_levels(own_key, extent, pieces, -0.22, 0.18)
    return jnp.clip(result, -bound, bound).astype(held_as)


def setup_inputs(seed: int = 0) -> dict:
    streams_of = jax.random.split(jax.random.key(seed), 8)
    tokens = gaussian(streams_of[0], (TOKENS, D), 1.0, 6.0, ((0, 8),))
    expert_ids_keys = jax.random.split(jax.random.fold_in(streams_of[1], 1), TOKENS // TOK_DEV)
    expert_ids_turns = jax.random.permutation(jax.random.fold_in(streams_of[1], 3), TOKENS // TOK_DEV)
    expert_ids = jax.vmap(lambda own, number: shared_out(jax.random.fold_in(streams_of[1], 2), own, number, TOK_DEV, EXPERTS, 2, CAP, 2))(expert_ids_keys, expert_ids_turns).reshape((TOKENS, 2))
    gate_weights = jnp.clip(0.2 + 0.8 * jax.random.uniform(streams_of[2], (TOKENS, 2), jnp.float32) ** shard_levels(streams_of[2], (TOKENS, 2), ((0, 8),), -0.2, 0.2), 0.2, 1.0)
    live_counts = draw_live_counts(jax.random.fold_in(streams_of[7], 71), 0)
    w_gate = gaussian(streams_of[4], (EXPERTS, D, FF), D ** -0.5, 0.09375, ((0, 4), (2, 8)))
    w_up = gaussian(streams_of[5], (EXPERTS, D, FF), D ** -0.5, 0.09375, ((0, 4), (2, 8)))
    w_down = gaussian(streams_of[6], (EXPERTS, FF, D), FF ** -0.5, 0.0625, ((0, 4), (1, 8)))
    return {"tokens": tokens, "expert_ids": expert_ids, "gate_weights": gate_weights, "live_counts": live_counts, "w_gate": w_gate, "w_up": w_up, "w_down": w_down}


def plan_routes(expert_ids, live_total, n_experts, capacity):
    row_count = expert_ids.shape[0]
    is_live = jnp.arange(row_count, dtype=jnp.int32) < live_total
    flat_ids = expert_ids.reshape(-1)
    live_pairs = jnp.repeat(is_live, 2)
    one_hot = ((flat_ids[:, None] == jnp.arange(n_experts, dtype=jnp.int32)[None, :]) & live_pairs[:, None]).astype(jnp.int32)
    earlier = jnp.cumsum(one_hot, axis=0) - one_hot
    slot_index = jnp.sum(earlier * one_hot, axis=1)
    targets = jnp.where(live_pairs, flat_ids * capacity + slot_index, -1).astype(jnp.int32)
    return targets.reshape(row_count, 2), jnp.sum(one_hot, axis=0)


def dispatch_rows(tokens, targets, slots_all):
    wanted = targets.reshape(-1)[None, :] == jnp.arange(slots_all, dtype=jnp.int32)[:, None]
    wanted = jnp.any(wanted.reshape(slots_all, -1, 2), axis=2).astype(jnp.bfloat16)
    return jnp.dot(wanted, tokens, preferred_element_type=jnp.float32).astype(jnp.bfloat16)


def combine_rows(results, targets, gate_weights):
    pick_index = jnp.maximum(targets, 0).astype(jnp.int32)
    selected = results[pick_index].astype(jnp.float32)
    weights = jnp.where(targets >= 0, gate_weights, jnp.zeros_like(gate_weights))
    return jnp.sum(weights[:, :, None] * selected, axis=1).astype(jnp.bfloat16)


def reference(tokens, expert_ids, gate_weights, live_counts, w_gate, w_up, w_down):
    tok_blocks = tokens.reshape(RANKS, TOK_DEV, D)
    id_blocks = expert_ids.reshape(RANKS, TOK_DEV, 2)
    gate_blocks = gate_weights.reshape(RANKS, TOK_DEV, 2)
    targets, loads = jax.vmap(lambda ids, live: plan_routes(ids, live, EXPERTS, CAP))(id_blocks, live_counts)
    outbound = jax.vmap(lambda toks, tgt: dispatch_rows(toks, tgt, EXPERTS * CAP))(tok_blocks, targets)
    per_expert = outbound.reshape(RANKS, EXPERTS, CAP, D).transpose(1, 0, 2, 3).reshape(EXPERTS, RANKS * CAP, D)
    shard_width = FF // N_DP

    def run_expert(operands):
        row_block, gate_matrix, up_matrix, down_matrix = operands
        total = jnp.zeros((row_block.shape[0], D), jnp.float32)
        for shard_index in range(N_DP):
            lower = shard_index * shard_width
            gate_act = jnp.dot(row_block, gate_matrix[:, lower:lower + shard_width], preferred_element_type=jnp.float32)
            up_act = jnp.dot(row_block, up_matrix[:, lower:lower + shard_width], preferred_element_type=jnp.float32)
            hidden = (jax.nn.silu(gate_act) * up_act).astype(jnp.bfloat16)
            partial_term = jnp.dot(hidden, down_matrix[lower:lower + shard_width, :], preferred_element_type=jnp.float32).astype(jnp.bfloat16)
            partial_term = lax.optimization_barrier(partial_term)
            total = total + partial_term.astype(jnp.float32)
        return total.astype(jnp.bfloat16)

    results = lax.map(run_expert, (per_expert, w_gate, w_up, w_down))
    returned = results.reshape(EXPERTS, RANKS, CAP, D).transpose(1, 0, 2, 3).reshape(RANKS, EXPERTS * CAP, D)
    mixed = jax.vmap(combine_rows)(returned, targets, gate_blocks).reshape(TOKENS, D)
    return mixed, jnp.sum(loads, axis=0).astype(jnp.int32)
```

```python
import functools

import jax
import jax.numpy as jnp
from jax import lax
from jax.experimental import pallas as pl
from jax.experimental.pallas import tpu as pltpu
from jax.sharding import PartitionSpec as P

MESH = pl.DeviceIdType.MESH
BF16, F32 = jnp.bfloat16, jnp.float32


def routing_weights(expert_ids, gate_weights, live_total, n_experts, my_expert):
    live = (jnp.arange(expert_ids.shape[0], dtype=jnp.int32) < live_total)[:, None]
    mine = (expert_ids == my_expert) & live
    weight = jnp.sum(jnp.where(mine, gate_weights, 0.0), axis=1)
    named = (expert_ids[:, :, None] == jnp.arange(n_experts, dtype=jnp.int32)) & live[:, :, None]
    return weight, jnp.sum(named.astype(jnp.int32), axis=(0, 1))


def general(tokens, expert_ids, gate_weights, live_counts, w_gate, w_up, w_down):
    weight, loads = routing_weights(
        expert_ids, gate_weights, live_counts[0], lax.axis_size("expert"), lax.axis_index("expert")
    )
    rows = lax.all_gather(tokens, "dp", axis=0, tiled=True)
    scale = lax.all_gather(weight, "dp", axis=0, tiled=True)[:, None]
    gate_act = jnp.dot(rows, w_gate[0], preferred_element_type=F32)
    up_act = jnp.dot(rows, w_up[0], preferred_element_type=F32)
    hidden = (jax.nn.silu(gate_act) * up_act * scale).astype(BF16)
    partial = jnp.dot(hidden, w_down[0], preferred_element_type=F32).astype(BF16)
    summed = lax.psum_scatter(partial, "dp", scatter_dimension=0, tiled=True)
    return lax.psum(summed, "expert"), lax.psum(loads, "dp")


def kernel(n_y, n_planes, n_experts, tokens, ids, gates, live, w_gate, w_up, w_down, out, totals,
           G, M, IDS, GATES, WG, WU, WD, H, Y, RC, RT, RS, RZ1, RL, RZ, OUT, send_sem, recv_sem, local_sem):
    dp, ex = lax.axis_index("dp"), lax.axis_index("expert")
    z, y = dp // n_y, dp % n_y
    x, c = ex // 2, ex % 2
    yo, xo, co = 1 - y, 1 - x, 1 - c
    n_dp = n_y * n_planes
    pieces, rows, width = G.shape[1:]
    half, quarter = pieces // 2, pieces // 4
    both, far = range(2), range(2, n_planes)

    low = z < n_planes // 2
    mid = (z > 0) & (z < n_planes - 1)
    near, beyond = jnp.where(low, 2, 1), jnp.where(low, n_planes - 1, 0)
    plane = [z, z + 1 - 2 * (z % 2), near, beyond]
    kind = jnp.where(mid, 0, 1)
    y_peer, x_peer, core_peer = (z * n_y + yo, ex), (dp, xo * 2 + c), (dp, x * 2 + co)
    z_peer = [(plane[k] * n_y + y, ex) for k in range(n_planes)]
    me = dp
    rank = [plane[k] * n_y + y for k in range(n_planes)]
    other = [plane[k] * n_y + yo for k in range(n_planes)]
    pair = [pl.ds(plane[k] * n_y, n_y) for k in range(n_planes)]
    member = [[plane[k] * n_y + j for j in range(n_y)] for k in range(n_planes)]
    dp_peers = [(lax.rem(dp + d, n_dp), ex) for d in range(1, n_dp)]
    peers = dp_peers + [x_peer, core_peer]
    barrier = pltpu.get_barrier_semaphore()

    n_local = [0]

    def local(src, dst):
        copy = pltpu.make_async_copy(src, dst, local_sem.at[n_local[0]])
        n_local[0] += 1
        copy.start()
        return copy

    route_loads = [local(ids, IDS), local(gates, GATES)]
    own_loads = [local(tokens.at[:, pl.ds(q * width, width)], G.at[me, q]) for q in range(pieces)]

    for a, b in peers:
        pl.semaphore_signal(barrier, inc=1, device_id={"dp": a, "expert": b}, device_id_type=MESH)

    weight_loads = [local(w_gate.at[0], WG), local(w_up.at[0], WU), local(w_down.at[0], WD)]

    sent = []

    def link(src, dst, to, slot=None):
        i = len(sent)
        copy = pltpu.make_async_remote_copy(
            src_ref=src, dst_ref=dst, send_sem=send_sem.at[i], recv_sem=recv_sem.at[i if slot is None else slot],
            device_id={"dp": to[0], "expert": to[1]}, device_id_type=MESH,
        )
        sent.append(copy)
        return copy

    def same(ref, to):
        return link(ref, ref, to)

    def arrival(ref, slot):
        return pltpu.make_async_remote_copy(
            src_ref=ref, dst_ref=ref, send_sem=send_sem.at[slot], recv_sem=recv_sem.at[slot],
            device_id={"dp": dp, "expert": ex}, device_id_type=MESH,
        )

    def go(*copies):
        for copy in copies:
            copy.start()

    def got(*copies):
        for copy in copies:
            copy.wait_recv()

    mine_c, other_c = pl.ds(c * half, half), pl.ds(co * half, half)
    P = [[c * half + h * quarter + o for o in range(quarter)] for h in range(2)]
    mx = [c * half + x * quarter + o for o in range(quarter)]
    ox = [c * half + xo * quarter + o for o in range(quarter)]

    metas = [same(M.at[me], peer) for peer in dp_peers]
    A0 = [same(G.at[me, mx[o]], y_peer) for o in both]
    B0 = [same(G.at[other[0], mx[o]], x_peer) for o in both]
    D0 = [same(G.at[other[0], mx[o]], core_peer) for o in both] + [same(G.at[other[0], ox[o]], core_peer) for o in both]

    def halves(k, o, by_y):
        if by_y:
            return [(rank[k], P[i][o]) for i in both]
        return [(member[k][i], mx[o]) for i in both]

    def hop(by_y):
        return y_peer if by_y else x_peer

    y_first = [None, (True, False), (False, True), (True, False)]
    Z1 = [[same(G.at[r, q], z_peer[1]) for r, q in halves(0, o, y_first[1][o])] for o in both]
    F1 = [[same(G.at[r, q], hop(y_first[1][o])) for r, q in halves(1, o, y_first[1][o])] for o in both]
    D1 = [
        [same(G.at[r, q], core_peer) for r, q in halves(1, o, y_first[1][o])]
        + [same(G.at[other[1], P[i][o]] if y_first[1][o] else G.at[member[1][i], ox[o]], core_peer) for i in both]
        for o in both
    ]
    ZS, GX, GY, GH, DZ, DF, DR = [[None, None] for _ in range(7)]
    first = len(sent)
    for k in far:
        ZS.append([link(G.at[me, mx[o]], G.at[me, mx[o]], z_peer[k], first + kind * 2 + o) for o in both])
    for k in far:
        near_x = [(other[k], mx[o]) if y_first[k][o] else (rank[k], ox[o]) for o in both]
        last_x = [(rank[k], ox[o]) if y_first[k][o] else (other[k], mx[o]) for o in both]
        GX.append([same(G.at[rank[k], mx[o]], x_peer) for o in both])
        GY.append([same(G.at[rank[k], mx[o]], y_peer) for o in both])
        GH.append([same(G.at[near_x[o]], x_peer if y_first[k][o] else y_peer) for o in both])
        DZ.append([same(G.at[rank[k], mx[o]], core_peer) for o in both])
        DF.append([same(G.at[near_x[o]], core_peer) for o in both])
        DR.append([[same(G.at[last_x[o]], core_peer), same(G.at[other[k], ox[o]], core_peer)] for o in both])
    ZG = [None, None] + [[arrival(G.at[me, mx[o]], first + (k - 2) * 2 + o) for o in both] for k in far]

    sum_y = [(True, False), (True, False), (False, True), (False, True)]
    C = [link(Y.at[pair[k], other_c], RC.at[k], core_peer) for k in range(n_planes)]
    T, TG, S = [], [], [None, None]
    for k in range(n_planes):
        T.append([
            [
                link(Y.at[other[k], P[i][o]], RT.at[k, o, i], y_peer)
                if sum_y[k][o]
                else link(Y.at[member[k][i], ox[o]], RT.at[k, o, i], x_peer)
                for i in both
            ]
            for o in both
        ])
        TG.append([halves(k, o, sum_y[k][o]) for o in both])
    for k in far:
        S.append([
            link(Y.at[rank[k], ox[o]], RS.at[k - 2, o], x_peer)
            if sum_y[k][o]
            else link(Y.at[other[k], mx[o]], RS.at[k - 2, o], y_peer)
            for o in both
        ])
    start = len(sent)
    ZR = [None, None] + [
        [link(Y.at[rank[k], mx[o]], RZ.at[kind, o], z_peer[k], start + kind * 2 + o) for o in both] for k in far
    ]
    ZA = [[arrival(RZ.at[i, o], start + i * 2 + o) for o in both] for i in both]
    ZR1 = [[link(Y.at[TG[1][o][i]], RZ1.at[o, i], z_peer[1]) for i in both] for o in both]
    L0 = [
        link(Y.at[me, ox[o]], RL.at[o], x_peer) if sum_y[0][o] else link(Y.at[other[0], mx[o]], RL.at[o], y_peer)
        for o in both
    ]
    FX = [same(OUT.at[mx[o]], x_peer) for o in both]
    FC = [same(OUT.at[mx[o]], core_peer) for o in both]
    LC = [same(OUT.at[ox[o]], core_peer) for o in both]

    for copy in route_loads:
        copy.wait()
    lane = lax.broadcasted_iota(jnp.int32, IDS.shape, 1)
    alive = lane < live[0]
    named = IDS[...]
    weight = jnp.sum(jnp.where((named == ex) & alive, GATES[...], 0.0), axis=0, keepdims=True)
    row = lax.broadcasted_iota(jnp.int32, M.shape[1:], 0)
    col = lax.broadcasted_iota(jnp.int32, M.shape[1:], 1)
    line = jnp.where(row == 0, weight, 0.0)
    for e in range(n_experts):
        count = jnp.sum(jnp.where((named == e) & alive, 1.0, 0.0))
        line = jnp.where((row == 1) & (col == e), count, line)
    M[me] = line

    for copy in own_loads:
        copy.wait()
    pl.semaphore_wait(barrier, len(peers))

    go(*metas)
    first_sends = [copy for o in both for copy in (A0[o], ZS[3][o], ZS[2][o])] + Z1[0]

    def st(i):
        go(first_sends[i])

    h_tile = min(256, WG.shape[1])

    def a0(o):
        got(A0[o])
        go(B0[o], D0[o])
        if o:
            go(*Z1[1])

    def b0(o):
        got(B0[o])
        go(D0[2 + o])

    def fz(o, i):
        got(Z1[o][i])
        go(F1[o][i], D1[o][i])

    def zg(k, o):
        got(ZG[k][o])
        go(*((GY[k][o], GX[k][o]) if y_first[k][o] else (GX[k][o], GY[k][o])), DZ[k][o])

    def gh(k, o):
        got((GX, GY)[y_first[k][o]][k][o])
        go(GH[k][o], DF[k][o])

    def f1(o, i):
        got(F1[o][i])
        go(D1[o][2 + i])

    def gb(k, o):
        got((GY, GX)[y_first[k][o]][k][o])
        go(DR[k][o][0])

    def gc(k, o):
        got(GH[k][o])
        go(DR[k][o][1])

    def whole(k):
        if k == 0:
            got(*D0)
        elif k == 1:
            got(*D1[0], *D1[1])
        else:
            got(*DZ[k], *DF[k], *DR[k][0], *DR[k][1])

    def tiles(tile, lo, hi):
        if hi - lo == 1:
            tile(lo)
        else:
            lax.fori_loop(lo, hi, lambda i, carry: (tile(i), carry)[1], 0, unroll=True)

    scales = {}

    def gate_up(k, lo, hi):
        if k not in scales:
            if not scales:
                got(*metas)
                weight_loads[0].wait()
                weight_loads[1].wait()
            columns = [jnp.transpose(M[member[k][j]])[:, 0:1] for j in range(n_y)]
            scales[k] = jnp.concatenate(columns, axis=0)

        def tile(t):
            cols = pl.ds(t * h_tile if isinstance(t, int) else pl.multiple_of(t * h_tile, h_tile), h_tile)
            lhs = jnp.concatenate([G[pair[k], q].reshape(n_y * rows, width) for q in range(pieces)], axis=1)
            g = jnp.dot(lhs, WG[:, cols], preferred_element_type=F32)
            u = jnp.dot(lhs, WU[:, cols], preferred_element_type=F32)
            H[k, :, cols] = (g / (1.0 + jnp.exp(-g)) * u * scales[k]).astype(BF16)

        tiles(tile, lo, hi)

    downs = []

    def down(k, lo, hi):
        if not downs:
            weight_loads[2].wait()
        downs.append(k)

        def tile(t):
            q = lax.rem(co * half + 2 * t, pieces)
            cols = pl.ds(pl.multiple_of(q * width, width), 2 * width)
            part = jnp.dot(H[k], WD[:, cols], preferred_element_type=F32).astype(BF16)
            for i in range(2):
                Y[pair[k], q + i] = part[:, i * width:(i + 1) * width].reshape(n_y, rows, width)

        tiles(tile, lo, hi)

    def add(r, q, value):
        Y[r, q] = (Y[r, q].astype(F32) + value.astype(F32)).astype(BF16)

    def r1(k):
        got(C[k])
        for j in range(n_y):
            def tile(q, carry):
                add(member[k][j], c * half + q, RC[k, j, q])
                return carry
            lax.fori_loop(0, half, tile, 0)
        go(T[k][0][0], T[k][1][0], T[k][0][1], T[k][1][1])

    def r2(k, o):
        for i in both:
            got(T[k][o][i])
            add(*TG[k][o][i], RT[k, o, i])
            if k == 1:
                go(ZR1[o][i])
        if k > 1:
            go(S[k][o])

    def r3(k, o):
        got(S[k][o])
        add(rank[k], mx[o], RS[k - 2, o])
        go(ZR[k][o])

    def rz1(o):
        for i in both:
            got(ZR1[o][i])
            add(*TG[0][o][i], RZ1[o, i])
        go(L0[o])

    def last(o):
        got(L0[o])
        total = Y[me, mx[o]].astype(F32) + RL[o].astype(F32)
        got(ZA[0][o], ZA[1][o])
        OUT[mx[o]] = (total + RZ[0, o].astype(F32) + RZ[1, o].astype(F32)).astype(BF16)
        go(FX[o], FC[o])
        store(mx[o])

    stores = []

    def store(q):
        stores.append(local(OUT.at[q], out.at[:, pl.ds(pl.multiple_of(q * width, width), width)]))

    def fin(o):
        got(FX[o])
        go(LC[o])
        store(ox[o])

    def loads():
        count = M[0]
        for r in range(1, n_dp):
            count = count + M[r]
        for e in range(n_experts):
            totals[e] = jnp.sum(jnp.where((row == 1) & (col == e), count, 0.0)).astype(jnp.int32)

    st(5)
    st(4)
    st(2)
    st(1)
    st(3)
    st(0)
    a0(1)
    a0(0)
    st(6)
    zg(3, 1)
    zg(3, 0)
    b0(1)
    gb(3, 1)
    b0(0)
    whole(0)
    gate_up(0, 0, 1)
    gh(3, 1)
    gh(3, 0)
    gate_up(0, 1, 2)
    st(7)
    gate_up(0, 2, 3)
    fz(1, 0)
    gate_up(0, 3, 4)
    zg(2, 1)
    gb(3, 0)
    gc(3, 0)
    gc(3, 1)
    whole(3)
    gate_up(3, 0, 1)
    fz(0, 0)
    fz(1, 1)
    gate_up(3, 1, 3)
    fz(0, 1)
    gh(2, 1)
    zg(2, 0)
    gate_up(3, 3, 4)
    down(3, 0, 2)
    go(C[3])
    down(3, 2, 4)
    r1(3)
    f1(0, 1)
    f1(1, 1)
    f1(0, 0)
    f1(1, 0)
    down(0, 0, 2)
    go(C[0])
    gb(2, 0)
    down(0, 2, 4)
    whole(1)
    gate_up(1, 0, 2)
    gc(2, 1)
    gh(2, 0)
    gb(2, 1)
    gate_up(1, 2, 3)
    r2(3, 1)
    gate_up(1, 3, 4)
    r2(3, 0)
    down(1, 0, 1)
    r1(0)
    down(1, 1, 2)
    go(C[1])
    down(1, 2, 4)
    gc(2, 0)
    r3(3, 1)
    r1(1)
    whole(2)
    gate_up(2, 0, 4)
    r3(3, 0)
    down(2, 0, 2)
    go(C[2])
    down(2, 2, 4)
    r2(1, 1)
    r1(2)
    r2(1, 0)
    r2(0, 1)
    r2(2, 1)
    r2(2, 0)
    r2(0, 0)
    r3(2, 1)
    r3(2, 0)
    rz1(1)
    rz1(0)
    loads()
    last(1)
    last(0)
    fin(1)
    fin(0)

    for o in both:
        got(FC[o])
        store(co * half + x * quarter + o)
    for o in both:
        got(LC[o])
        store(co * half + xo * quarter + o)
    for copy in stores:
        copy.wait()
    for copy in sent:
        copy.wait_send()


def planned(n_y, n_planes, tokens, expert_ids, gate_weights, live_counts, w_gate, w_up, w_down):
    n_experts = lax.axis_size("expert")
    rows, model = tokens.shape
    hidden = w_gate.shape[2]
    n_dp, pieces = n_y * n_planes, 8
    width, half, quarter = model // pieces, pieces // 2, pieces // 4
    hbm = pl.BlockSpec(memory_space=pl.ANY)
    smem = pl.BlockSpec(memory_space=pltpu.SMEM)
    return pl.pallas_call(
        functools.partial(kernel, n_y, n_planes, n_experts),
        name="moe",
        out_shape=(jax.ShapeDtypeStruct((rows, model), BF16), jax.ShapeDtypeStruct((n_experts,), jnp.int32)),
        in_specs=[hbm] * 3 + [smem] + [hbm] * 3,
        out_specs=(hbm, smem),
        scratch_shapes=[
            pltpu.VMEM((n_dp, pieces, rows, width), BF16),
            pltpu.VMEM((n_dp, 8, rows), F32),
            pltpu.VMEM((2, rows), jnp.int32),
            pltpu.VMEM((2, rows), F32),
            pltpu.VMEM((model, hidden), BF16),
            pltpu.VMEM((model, hidden), BF16),
            pltpu.VMEM((hidden, model), BF16),
            pltpu.VMEM((n_planes, n_y * rows, hidden), BF16),
            pltpu.VMEM((n_dp, pieces, rows, width), BF16),
            pltpu.VMEM((n_planes, n_y, half, rows, width), BF16),
            pltpu.VMEM((n_planes, 2, 2, rows, width), BF16),
            pltpu.VMEM((2, 2, rows, width), BF16),
            pltpu.VMEM((2, 2, rows, width), BF16),
            pltpu.VMEM((2, rows, width), BF16),
            pltpu.VMEM((2, 2, rows, width), BF16),
            pltpu.VMEM((pieces, rows, width), BF16),
            pltpu.SemaphoreType.DMA((128,)),
            pltpu.SemaphoreType.DMA((128,)),
            pltpu.SemaphoreType.DMA((32,)),
        ],
        compiler_params=pltpu.CompilerParams(
            collective_id=0, has_side_effects=True, vmem_limit_bytes=63 * 2**20
        ),
    )(tokens, expert_ids.T, gate_weights.T, live_counts, w_gate, w_up, w_down)


def solution(mesh):
    n_dp, n_experts = mesh.shape["dp"], mesh.shape["expert"]
    n_x = n_experts // 2
    n_y = n_x
    n_planes = n_dp // n_y
    body = general
    if n_y == 2 and n_planes == 4:
        body = functools.partial(planned, n_y, n_planes)
    placed = (
        P("dp", None),
        P("dp", None),
        P("dp", None),
        P("dp"),
        P("expert", None, "dp"),
        P("expert", None, "dp"),
        P("expert", "dp", None),
    )
    return jax.shard_map(
        body, mesh=mesh, in_specs=placed, out_specs=(P("dp", None), P()), check_vma=False
    )
```

```python
import functools

import jax
import jax.numpy as jnp
from jax import lax
from jax.experimental import pallas as pl
from jax.experimental.pallas import tpu as pltpu
from jax.sharding import PartitionSpec as P

MESH = pl.DeviceIdType.MESH
BF16, F32 = jnp.bfloat16, jnp.float32


def routing_weights(expert_ids, gate_weights, live_total, n_experts, my_expert):
    live = (jnp.arange(expert_ids.shape[0], dtype=jnp.int32) < live_total)[:, None]
    mine = (expert_ids == my_expert) & live
    weight = jnp.sum(jnp.where(mine, gate_weights, 0.0), axis=1)
    named = (expert_ids[:, :, None] == jnp.arange(n_experts, dtype=jnp.int32)) & live[:, :, None]
    return weight, jnp.sum(named.astype(jnp.int32), axis=(0, 1))


def general(tokens, expert_ids, gate_weights, live_counts, w_gate, w_up, w_down):
    weight, loads = routing_weights(
        expert_ids, gate_weights, live_counts[0], lax.axis_size("expert"), lax.axis_index("expert")
    )
    rows = lax.all_gather(tokens, "dp", axis=0, tiled=True)
    scale = lax.all_gather(weight, "dp", axis=0, tiled=True)[:, None]
    gate_act = jnp.dot(rows, w_gate[0], preferred_element_type=F32)
    up_act = jnp.dot(rows, w_up[0], preferred_element_type=F32)
    hidden = (jax.nn.silu(gate_act) * up_act * scale).astype(BF16)
    partial = jnp.dot(hidden, w_down[0], preferred_element_type=F32).astype(BF16)
    summed = lax.psum_scatter(partial, "dp", scatter_dimension=0, tiled=True)
    return lax.psum(summed, "expert"), lax.psum(loads, "dp")


def kernel(n_y, n_planes, n_experts, tokens, ids, gates, live, w_gate, w_up, w_down, OUT, LOADS,
           G, M, IDS, GATES, WG, WU, WD, H, Y, RC, RT, RS, RZ1, RL, RZ, send_sem, recv_sem, local_sem):
    dp, ex = lax.axis_index("dp"), lax.axis_index("expert")
    z, y = dp // n_y, dp % n_y
    x, c = ex // 2, ex % 2
    yo, xo, co = 1 - y, 1 - x, 1 - c
    n_dp = n_y * n_planes
    pieces, rows, width = G.shape[1:]
    half, quarter = pieces // 2, pieces // 4
    both, far, parts = range(2), range(2, n_planes), range(quarter)

    low = z < n_planes // 2
    mid = (z > 0) & (z < n_planes - 1)
    near, beyond = jnp.where(low, 2, 1), jnp.where(low, n_planes - 1, 0)
    plane = [z, z + 1 - 2 * (z % 2), near, beyond]
    kind = jnp.where(mid, 0, 1)
    y_peer, x_peer, core_peer = (z * n_y + yo, ex), (dp, xo * 2 + c), (dp, x * 2 + co)
    z_peer = [(plane[k] * n_y + y, ex) for k in range(n_planes)]
    me = dp
    rank = [plane[k] * n_y + y for k in range(n_planes)]
    other = [plane[k] * n_y + yo for k in range(n_planes)]
    pair = [pl.ds(plane[k] * n_y, n_y) for k in range(n_planes)]
    member = [[plane[k] * n_y + j for j in range(n_y)] for k in range(n_planes)]
    dp_peers = [(lax.rem(dp + d, n_dp), ex) for d in range(1, n_dp)]
    peers = dp_peers + [x_peer, core_peer]
    barrier = pltpu.get_barrier_semaphore()

    n_local = [0]

    def local(src, dst):
        copy = pltpu.make_async_copy(src, dst, local_sem.at[n_local[0]])
        n_local[0] += 1
        copy.start()
        return copy

    route_loads = [local(ids, IDS), local(gates, GATES)]
    own_loads = [local(tokens.at[:, pl.ds(q * width, width)], G.at[me, q]) for q in range(pieces)]

    for a, b in peers:
        pl.semaphore_signal(barrier, inc=1, device_id={"dp": a, "expert": b}, device_id_type=MESH)

    weight_loads = [local(w_gate.at[0], WG), local(w_up.at[0], WU), local(w_down.at[0], WD)]

    sent = []

    def link(src, dst, to, slot=None):
        i = len(sent)
        copy = pltpu.make_async_remote_copy(
            src_ref=src, dst_ref=dst, send_sem=send_sem.at[i], recv_sem=recv_sem.at[i if slot is None else slot],
            device_id={"dp": to[0], "expert": to[1]}, device_id_type=MESH,
        )
        sent.append(copy)
        return copy

    def same(ref, to):
        return link(ref, ref, to)

    def arrival(ref, slot):
        return pltpu.make_async_remote_copy(
            src_ref=ref, dst_ref=ref, send_sem=send_sem.at[slot], recv_sem=recv_sem.at[slot],
            device_id={"dp": dp, "expert": ex}, device_id_type=MESH,
        )

    def go(*copies):
        for copy in copies:
            copy.start()

    def got(*copies):
        for copy in copies:
            copy.wait_recv()

    mine_c, other_c = pl.ds(c * half, half), pl.ds(co * half, half)
    P = [[c * half + h * quarter + o for o in range(quarter)] for h in range(2)]
    mx = [c * half + x * quarter + o for o in range(quarter)]
    ox = [c * half + xo * quarter + o for o in range(quarter)]

    metas = [same(M.at[me], peer) for peer in dp_peers]
    A0 = [same(G.at[me, mx[o]], y_peer) for o in parts]
    B0 = [same(G.at[other[0], mx[o]], x_peer) for o in parts]
    D0 = [[same(G.at[other[0], q[o]], core_peer) for o in parts] for q in (mx, ox)]

    def halves(k, o, by_y):
        if by_y:
            return [(rank[k], P[i][o]) for i in both]
        return [(member[k][i], mx[o]) for i in both]

    def hop(by_y):
        return y_peer if by_y else x_peer

    y_first = [None, (False, False, True, True), (False, False, True, True), (True, True, False, False)]
    Z1 = [[same(G.at[r, q], z_peer[1]) for r, q in halves(0, o, y_first[1][o])] for o in parts]
    F1 = [[same(G.at[r, q], hop(y_first[1][o])) for r, q in halves(1, o, y_first[1][o])] for o in parts]
    D1 = [
        [same(G.at[r, q], core_peer) for r, q in halves(1, o, y_first[1][o])]
        + [same(G.at[other[1], P[i][o]] if y_first[1][o] else G.at[member[1][i], ox[o]], core_peer) for i in both]
        for o in parts
    ]
    ZS, GX, GY, GH, DZ, DF, DR = [[None, None] for _ in range(7)]
    first = len(sent)
    for k in far:
        ZS.append([link(G.at[me, mx[o]], G.at[me, mx[o]], z_peer[k], first + kind * quarter + o) for o in parts])
    for k in far:
        near_x = [(other[k], mx[o]) if y_first[k][o] else (rank[k], ox[o]) for o in parts]
        last_x = [(rank[k], ox[o]) if y_first[k][o] else (other[k], mx[o]) for o in parts]
        GX.append([same(G.at[rank[k], mx[o]], x_peer) for o in parts])
        GY.append([same(G.at[rank[k], mx[o]], y_peer) for o in parts])
        GH.append([same(G.at[near_x[o]], x_peer if y_first[k][o] else y_peer) for o in parts])
        DZ.append([same(G.at[rank[k], mx[o]], core_peer) for o in parts])
        DF.append([same(G.at[near_x[o]], core_peer) for o in parts])
        DR.append([[same(G.at[last_x[o]], core_peer), same(G.at[other[k], ox[o]], core_peer)] for o in parts])
    ZG = [None, None] + [[arrival(G.at[me, mx[o]], first + (k - 2) * quarter + o) for o in parts] for k in far]

    sum_y = [(True, True, False, False), (True, True, False, False), (True, True, False, False), (True, True, False, False)]
    C = [link(Y.at[pair[k], other_c], RC.at[k], core_peer) for k in range(n_planes)]
    T, TG, S = [], [], [None, None]
    for k in range(n_planes):
        T.append([
            [
                link(Y.at[other[k], P[i][o]], RT.at[k, o, i], y_peer)
                if sum_y[k][o]
                else link(Y.at[member[k][i], ox[o]], RT.at[k, o, i], x_peer)
                for i in both
            ]
            for o in parts
        ])
        TG.append([halves(k, o, sum_y[k][o]) for o in parts])
    for k in far:
        S.append([
            link(Y.at[rank[k], ox[o]], RS.at[k - 2, o], x_peer)
            if sum_y[k][o]
            else link(Y.at[other[k], mx[o]], RS.at[k - 2, o], y_peer)
            for o in parts
        ])
    start = len(sent)
    ZR = [None, None] + [
        [link(Y.at[rank[k], mx[o]], RZ.at[kind, o], z_peer[k], start + kind * quarter + o) for o in parts] for k in far
    ]
    ZA = [[arrival(RZ.at[i, o], start + i * quarter + o) for o in parts] for i in both]
    ZR1 = [[link(Y.at[TG[1][o][i]], RZ1.at[o, i], z_peer[1]) for i in both] for o in parts]
    L0 = [
        link(Y.at[me, ox[o]], RL.at[o], x_peer) if sum_y[0][o] else link(Y.at[other[0], mx[o]], RL.at[o], y_peer)
        for o in parts
    ]
    FX = [same(OUT.at[mx[o]], x_peer) for o in parts]
    FC = [same(OUT.at[mx[o]], core_peer) for o in parts]
    LC = [same(OUT.at[ox[o]], core_peer) for o in parts]

    for copy in route_loads:
        copy.wait()
    lane = lax.broadcasted_iota(jnp.int32, IDS.shape, 1)
    alive = lane < live[0]
    named = IDS[...]
    weight = jnp.sum(jnp.where((named == ex) & alive, GATES[...], 0.0), axis=0, keepdims=True)
    row = lax.broadcasted_iota(jnp.int32, M.shape[1:], 0)
    col = lax.broadcasted_iota(jnp.int32, M.shape[1:], 1)
    line = jnp.where(row == 0, weight, 0.0)
    for e in range(n_experts):
        count = jnp.sum(jnp.where((named == e) & alive, 1.0, 0.0))
        line = jnp.where((row == 1) & (col == e), count, line)
    M[me] = line

    for copy in own_loads:
        copy.wait()
    pl.semaphore_wait(barrier, len(peers))

    go(*metas)
    first_sends = [copy for o in parts for copy in (A0[o], ZS[3][o], ZS[2][o])]
    first_sends += [copy for o in parts if y_first[1][o] for copy in Z1[o]]

    def st(i):
        go(first_sends[i])

    h_tile = min(256, WG.shape[1])

    def a0(o):
        got(A0[o])
        go(B0[o], D0[0][o])
        if not y_first[1][o]:
            go(*Z1[o])

    def b0(o):
        got(B0[o])
        go(D0[1][o])

    def fz(o, i):
        got(Z1[o][i])
        go(F1[o][i], D1[o][i])

    def zg(k, o):
        got(ZG[k][o])
        go(*((GY[k][o], GX[k][o]) if y_first[k][o] else (GX[k][o], GY[k][o])), DZ[k][o])

    def gh(k, o):
        got((GX, GY)[y_first[k][o]][k][o])
        go(GH[k][o], DF[k][o])

    def f1(o, i):
        got(F1[o][i])
        go(D1[o][2 + i])

    def gb(k, o):
        got((GY, GX)[y_first[k][o]][k][o])
        go(DR[k][o][0])

    def gc(k, o):
        got(GH[k][o])
        go(DR[k][o][1])

    def whole(k):
        if k == 0:
            got(*D0[0], *D0[1])
        elif k == 1:
            got(*[copy for o in parts for copy in D1[o]])
        else:
            got(*DZ[k], *DF[k], *[copy for o in parts for copy in DR[k][o]])

    def tiles(tile, lo, hi):
        if hi - lo == 1:
            tile(lo)
        else:
            lax.fori_loop(lo, hi, lambda i, carry: (tile(i), carry)[1], 0, unroll=True)

    scales = {}

    def gate_up(k, lo, hi):
        if k not in scales:
            if not scales:
                got(*metas)
                weight_loads[0].wait()
                weight_loads[1].wait()
            columns = [jnp.transpose(M[member[k][j]])[:, 0:1] for j in range(n_y)]
            scales[k] = jnp.concatenate(columns, axis=0)

        def tile(t):
            cols = pl.ds(t * h_tile if isinstance(t, int) else pl.multiple_of(t * h_tile, h_tile), h_tile)
            lhs = jnp.concatenate([G[pair[k], q].reshape(n_y * rows, width) for q in range(pieces)], axis=1)
            g = jnp.dot(lhs, WG[:, cols], preferred_element_type=F32)
            u = jnp.dot(lhs, WU[:, cols], preferred_element_type=F32)
            H[k, :, cols] = (g / (1.0 + jnp.exp(-g)) * u * scales[k]).astype(BF16)

        tiles(tile, lo, hi)

    downs, per = [], pieces // 4

    def down(k, lo, hi):
        if not downs:
            weight_loads[2].wait()
        downs.append(k)

        def tile(t):
            q = lax.rem(co * half + per * t, pieces)
            cols = pl.ds(pl.multiple_of(q * width, width), per * width)
            part = jnp.dot(H[k], WD[:, cols], preferred_element_type=F32).astype(BF16)
            for i in range(per):
                Y[pair[k], q + i] = part[:, i * width:(i + 1) * width].reshape(n_y, rows, width)

        tiles(tile, lo, hi)

    def add(r, q, value):
        Y[r, q] = (Y[r, q].astype(F32) + value.astype(F32)).astype(BF16)

    def r1(k):
        got(C[k])
        for j in range(n_y):
            def tile(q, carry):
                add(member[k][j], c * half + q, RC[k, j, q])
                return carry
            lax.fori_loop(0, half, tile, 0)
        go(*[T[k][o][i] for i in both for o in parts])

    def r2(k, o):
        for i in both:
            got(T[k][o][i])
            add(*TG[k][o][i], RT[k, o, i])
            if k == 1:
                go(ZR1[o][i])
        if k > 1:
            go(S[k][o])

    def r3(k, o):
        got(S[k][o])
        add(rank[k], mx[o], RS[k - 2, o])
        go(ZR[k][o])

    def rz1(o):
        for i in both:
            got(ZR1[o][i])
            add(*TG[0][o][i], RZ1[o, i])
        go(L0[o])

    def last(o):
        got(L0[o])
        total = Y[me, mx[o]].astype(F32) + RL[o].astype(F32)
        got(ZA[0][o], ZA[1][o])
        OUT[mx[o]] = (total + RZ[0, o].astype(F32) + RZ[1, o].astype(F32)).astype(BF16)
        go(FX[o], FC[o])

    def fin(o):
        got(FX[o])
        go(LC[o])

    def loads():
        count = M[0]
        for r in range(1, n_dp):
            count = count + M[r]
        LOADS[...] = count

    st(9)
    st(2)
    st(6)
    st(1)
    st(0)
    st(7)
    st(3)
    st(10)
    st(8)
    a0(3)
    st(4)
    st(11)
    a0(2)
    st(5)
    zg(3, 0)
    st(14)
    a0(0)
    a0(1)
    zg(3, 2)
    zg(3, 1)
    b0(2)
    b0(3)
    gh(3, 2)
    b0(1)
    b0(0)
    whole(0)
    zg(3, 3)
    gh(3, 0)
    gate_up(0, 0, 2)
    zg(2, 0)
    gb(3, 0)
    st(13)
    gate_up(0, 2, 3)
    gh(3, 3)
    gb(3, 2)
    gh(3, 1)
    gc(3, 2)
    gate_up(0, 3, 4)
    st(12)
    st(15)
    zg(2, 2)
    down(0, 0, 1)
    fz(1, 0)
    gb(3, 3)
    fz(3, 0)
    gc(3, 0)
    gb(3, 1)
    gc(3, 3)
    gc(3, 1)
    down(0, 1, 2)
    go(C[0])
    fz(1, 1)
    fz(0, 0)
    zg(2, 3)
    whole(3)
    gate_up(3, 0, 1)
    fz(2, 1)
    fz(0, 1)
    gate_up(3, 1, 2)
    fz(2, 0)
    gate_up(3, 2, 3)
    fz(3, 1)
    f1(1, 1)
    gh(2, 0)
    gh(2, 2)
    gate_up(3, 3, 4)
    gh(2, 3)
    f1(3, 0)
    down(3, 0, 2)
    go(C[3])
    zg(2, 1)
    down(3, 2, 3)
    f1(1, 0)
    down(0, 2, 3)
    f1(2, 1)
    f1(0, 0)
    f1(0, 1)
    f1(2, 0)
    down(3, 3, 4)
    r1(3)
    f1(3, 1)
    down(0, 3, 4)
    gc(2, 2)
    whole(1)
    gate_up(1, 0, 1)
    gc(2, 0)
    gc(2, 3)
    gh(2, 1)
    gate_up(1, 1, 4)
    r2(3, 0)
    gb(2, 0)
    r2(3, 2)
    down(1, 0, 2)
    go(C[1])
    r2(3, 1)
    gb(2, 1)
    gb(2, 3)
    r2(3, 3)
    down(1, 2, 3)
    gb(2, 2)
    r3(3, 0)
    r1(0)
    gc(2, 1)
    down(1, 3, 4)
    r1(1)
    whole(2)
    gate_up(2, 0, 1)
    r3(3, 1)
    gate_up(2, 1, 3)
    r3(3, 2)
    gate_up(2, 3, 4)
    down(2, 0, 2)
    go(C[2])
    r2(0, 0)
    down(2, 2, 3)
    r2(1, 2)
    down(2, 3, 4)
    r1(2)
    r3(3, 3)
    r2(1, 0)
    r2(1, 3)
    r2(2, 2)
    r2(0, 2)
    r2(2, 3)
    r2(2, 0)
    r3(2, 2)
    r2(1, 1)
    r2(2, 1)
    rz1(0)
    r2(0, 1)
    r3(2, 0)
    r3(2, 3)
    rz1(2)
    r2(0, 3)
    loads()
    last(2)
    rz1(1)
    rz1(3)
    r3(2, 1)
    last(0)
    last(3)
    last(1)
    fin(3)
    fin(2)
    fin(0)
    fin(1)

    for o in parts:
        got(FC[o], LC[o])
    for copy in sent:
        copy.wait_send()


def collect(values, loads, out, totals, sem):
    pieces, _, width = values.shape
    copies = [
        pltpu.make_async_copy(values.at[q], out.at[:, pl.ds(q * width, width)], sem.at[q]) for q in range(pieces)
    ]
    for copy in copies:
        copy.start()
    row = lax.broadcasted_iota(jnp.int32, loads.shape, 0)
    col = lax.broadcasted_iota(jnp.int32, loads.shape, 1)
    for e in range(totals.shape[0]):
        totals[e] = jnp.sum(jnp.where((row == 1) & (col == e), loads[...], 0.0)).astype(jnp.int32)
    for copy in copies:
        copy.wait()


def planned(n_y, n_planes, tokens, expert_ids, gate_weights, live_counts, w_gate, w_up, w_down):
    n_experts = lax.axis_size("expert")
    rows, model = tokens.shape
    hidden = w_gate.shape[2]
    n_dp, pieces = n_y * n_planes, 16
    width, half, quarter = model // pieces, pieces // 2, pieces // 4
    hbm = pl.BlockSpec(memory_space=pl.ANY)
    smem = pl.BlockSpec(memory_space=pltpu.SMEM)
    vmem = pl.BlockSpec(memory_space=pltpu.VMEM)
    values, loads = pl.pallas_call(
        functools.partial(kernel, n_y, n_planes, n_experts),
        name="moe",
        out_shape=(pltpu.VMEM((pieces, rows, width), BF16), pltpu.VMEM((8, rows), F32)),
        in_specs=[hbm] * 3 + [smem] + [hbm] * 3,
        out_specs=(vmem, vmem),
        scratch_shapes=[
            pltpu.VMEM((n_dp, pieces, rows, width), BF16),
            pltpu.VMEM((n_dp, 8, rows), F32),
            pltpu.VMEM((2, rows), jnp.int32),
            pltpu.VMEM((2, rows), F32),
            pltpu.VMEM((model, hidden), BF16),
            pltpu.VMEM((model, hidden), BF16),
            pltpu.VMEM((hidden, model), BF16),
            pltpu.VMEM((n_planes, n_y * rows, hidden), BF16),
            pltpu.VMEM((n_dp, pieces, rows, width), BF16),
            pltpu.VMEM((n_planes, n_y, half, rows, width), BF16),
            pltpu.VMEM((n_planes, quarter, 2, rows, width), BF16),
            pltpu.VMEM((2, quarter, rows, width), BF16),
            pltpu.VMEM((quarter, 2, rows, width), BF16),
            pltpu.VMEM((quarter, rows, width), BF16),
            pltpu.VMEM((2, quarter, rows, width), BF16),
            pltpu.SemaphoreType.DMA((224,)),
            pltpu.SemaphoreType.DMA((224,)),
            pltpu.SemaphoreType.DMA((64,)),
        ],
        compiler_params=pltpu.CompilerParams(
            collective_id=0, has_side_effects=True, vmem_limit_bytes=56 * 2**20
        ),
    )(tokens, expert_ids.T, gate_weights.T, live_counts, w_gate, w_up, w_down)
    return pl.pallas_call(
        collect,
        name="collect",
        out_shape=(jax.ShapeDtypeStruct((rows, model), BF16), jax.ShapeDtypeStruct((n_experts,), jnp.int32)),
        in_specs=[vmem, vmem],
        out_specs=(hbm, smem),
        scratch_shapes=[pltpu.SemaphoreType.DMA((pieces,))],
        compiler_params=pltpu.CompilerParams(vmem_limit_bytes=4 * 2**20),
    )(values, loads)


def solution(mesh):
    n_dp, n_experts = mesh.shape["dp"], mesh.shape["expert"]
    n_x = n_experts // 2
    n_y = n_x
    n_planes = n_dp // n_y
    body = general
    if n_y == 2 and n_planes == 4:
        body = functools.partial(planned, n_y, n_planes)
    placed = (
        P("dp", None),
        P("dp", None),
        P("dp", None),
        P("dp"),
        P("expert", None, "dp"),
        P("expert", None, "dp"),
        P("expert", "dp", None),
    )
    return jax.shard_map(
        body, mesh=mesh, in_specs=placed, out_specs=(P("dp", None), P()), check_vma=False
    )
```

```python
import functools

import jax
import jax.numpy as jnp
from jax import lax
from jax.experimental import pallas as pl
from jax.experimental.pallas import tpu as pltpu
from jax.sharding import PartitionSpec as P

MESH = pl.DeviceIdType.MESH
BF16, F32 = jnp.bfloat16, jnp.float32


def routing_weights(expert_ids, gate_weights, live_total, n_experts, my_expert):
    live = (jnp.arange(expert_ids.shape[0], dtype=jnp.int32) < live_total)[:, None]
    mine = (expert_ids == my_expert) & live
    weight = jnp.sum(jnp.where(mine, gate_weights, 0.0), axis=1)
    named = (expert_ids[:, :, None] == jnp.arange(n_experts, dtype=jnp.int32)) & live[:, :, None]
    return weight, jnp.sum(named.astype(jnp.int32), axis=(0, 1))


def general(tokens, expert_ids, gate_weights, live_counts, w_gate, w_up, w_down):
    weight, loads = routing_weights(
        expert_ids, gate_weights, live_counts[0], lax.axis_size("expert"), lax.axis_index("expert")
    )
    rows = lax.all_gather(tokens, "dp", axis=0, tiled=True)
    scale = lax.all_gather(weight, "dp", axis=0, tiled=True)[:, None]
    gate_act = jnp.dot(rows, w_gate[0], preferred_element_type=F32)
    up_act = jnp.dot(rows, w_up[0], preferred_element_type=F32)
    hidden = (jax.nn.silu(gate_act) * up_act * scale).astype(BF16)
    partial = jnp.dot(hidden, w_down[0], preferred_element_type=F32).astype(BF16)
    summed = lax.psum_scatter(partial, "dp", scatter_dimension=0, tiled=True)
    return lax.psum(summed, "expert"), lax.psum(loads, "dp")


def kernel(n_y, n_planes, n_experts, tokens, ids, gates, live, w_gate, w_up, w_down, OUT, LOADS,
           G, M, IDS, GATES, WG, WU, WD, H, Y, RC, RT, RS, RZ1, RE, RZ, send_sem, recv_sem, local_sem):
    dp, ex = lax.axis_index("dp"), lax.axis_index("expert")
    z, y = dp // n_y, dp % n_y
    x, c = ex // 2, ex % 2
    yo, xo, co = 1 - y, 1 - x, 1 - c
    n_dp = n_y * n_planes
    pieces, rows, width = G.shape[1:]
    half, quarter = pieces // 2, pieces // 4
    both, far, parts = range(2), range(2, n_planes), range(quarter)

    low = z < n_planes // 2
    mid = (z > 0) & (z < n_planes - 1)
    near, beyond = jnp.where(low, 2, 1), jnp.where(low, n_planes - 1, 0)
    plane = [z, z + 1 - 2 * (z % 2), near, beyond]
    kind = jnp.where(mid, 0, 1)
    y_peer, x_peer, core_peer = (z * n_y + yo, ex), (dp, xo * 2 + c), (dp, x * 2 + co)
    z_peer = [(plane[k] * n_y + y, ex) for k in range(n_planes)]
    me = dp
    rank = [plane[k] * n_y + y for k in range(n_planes)]
    other = [plane[k] * n_y + yo for k in range(n_planes)]
    pair = [pl.ds(plane[k] * n_y, n_y) for k in range(n_planes)]
    member = [[plane[k] * n_y + j for j in range(n_y)] for k in range(n_planes)]
    dp_peers = [(lax.rem(dp + d, n_dp), ex) for d in range(1, n_dp)]
    peers = dp_peers + [x_peer, core_peer]
    barrier = pltpu.get_barrier_semaphore()

    n_local = [0]

    def local(src, dst):
        copy = pltpu.make_async_copy(src, dst, local_sem.at[n_local[0]])
        n_local[0] += 1
        copy.start()
        return copy

    route_loads = [local(ids, IDS), local(gates, GATES)]
    own_loads = [local(tokens.at[:, pl.ds(q * width, width)], G.at[me, q]) for q in range(pieces)]

    for a, b in peers:
        pl.semaphore_signal(barrier, inc=1, device_id={"dp": a, "expert": b}, device_id_type=MESH)

    weight_loads = [local(w_gate.at[0], WG), local(w_up.at[0], WU), local(w_down.at[0], WD)]

    sent = []

    def link(src, dst, to, slot=None):
        i = len(sent)
        copy = pltpu.make_async_remote_copy(
            src_ref=src, dst_ref=dst, send_sem=send_sem.at[i], recv_sem=recv_sem.at[i if slot is None else slot],
            device_id={"dp": to[0], "expert": to[1]}, device_id_type=MESH,
        )
        sent.append(copy)
        return copy

    def same(ref, to):
        return link(ref, ref, to)

    def arrival(ref, slot):
        return pltpu.make_async_remote_copy(
            src_ref=ref, dst_ref=ref, send_sem=send_sem.at[slot], recv_sem=recv_sem.at[slot],
            device_id={"dp": dp, "expert": ex}, device_id_type=MESH,
        )

    def go(*copies):
        for copy in copies:
            copy.start()

    def got(*copies):
        for copy in copies:
            copy.wait_recv()

    mx = [c * half + x * quarter + o for o in range(quarter)]
    ox = [c * half + xo * quarter + o for o in range(quarter)]

    metas = [same(M.at[me], peer) for peer in dp_peers]
    A0 = [same(G.at[me, mx[o]], y_peer) for o in parts]
    B0 = [same(G.at[other[0], mx[o]], x_peer) for o in parts]
    D0 = [[same(G.at[other[0], q[o]], core_peer) for o in parts] for q in (mx, ox)]

    def halves(k, o, by_y):
        if by_y:
            return [(rank[k], ox[o]), (rank[k], mx[o])]
        return [(member[k][i], mx[o]) for i in both]

    def hop(by_y):
        return y_peer if by_y else x_peer

    y_first = [None, (False, False, True, True), (False, False, True, True), (True, True, False, False)]
    Z1 = [[same(G.at[r, q], z_peer[1]) for r, q in halves(0, o, y_first[1][o])] for o in parts]
    F1 = [[same(G.at[r, q], hop(y_first[1][o])) for r, q in halves(1, o, y_first[1][o])] for o in parts]
    D1 = [
        [same(G.at[r, q], core_peer) for r, q in halves(1, o, y_first[1][o])]
        + [same(G.at[other[1], (ox, mx)[i][o]] if y_first[1][o] else G.at[member[1][i], ox[o]], core_peer) for i in both]
        for o in parts
    ]
    ZS, GX, GY, GH, DZ, DF, DR = [[None, None] for _ in range(7)]
    first = len(sent)
    for k in far:
        ZS.append([link(G.at[me, mx[o]], G.at[me, mx[o]], z_peer[k], first + kind * quarter + o) for o in parts])
    for k in far:
        near_x = [(other[k], mx[o]) if y_first[k][o] else (rank[k], ox[o]) for o in parts]
        last_x = [(rank[k], ox[o]) if y_first[k][o] else (other[k], mx[o]) for o in parts]
        GX.append([same(G.at[rank[k], mx[o]], x_peer) for o in parts])
        GY.append([same(G.at[rank[k], mx[o]], y_peer) for o in parts])
        GH.append([same(G.at[near_x[o]], x_peer if y_first[k][o] else y_peer) for o in parts])
        DZ.append([same(G.at[rank[k], mx[o]], core_peer) for o in parts])
        DF.append([same(G.at[near_x[o]], core_peer) for o in parts])
        DR.append([[same(G.at[last_x[o]], core_peer), same(G.at[other[k], ox[o]], core_peer)] for o in parts])
    ZG = [None, None] + [[arrival(G.at[me, mx[o]], first + (k - 2) * quarter + o) for o in parts] for k in far]

    sum_y = [(True, True, False, False), (True, True, False, False), (True, True, False, False), (True, True, False, False)]
    sides = [xo * quarter, x * quarter]
    C = [
        [
            link(Y.at[pair[k], pl.ds(co * half + side, quarter)], RC.at[k, :, pl.ds(side, quarter)], core_peer)
            for side in sides
        ]
        for k in range(n_planes)
    ]
    T, TG, S = [], [], [None, None]
    for k in range(n_planes):
        T.append([
            [
                link(Y.at[other[k], (ox, mx)[i][o]], RT.at[k, o, i], y_peer)
                if sum_y[k][o]
                else link(Y.at[member[k][i], ox[o]], RT.at[k, o, i], x_peer)
                for i in both
            ]
            for o in parts
        ])
        TG.append([halves(k, o, sum_y[k][o]) for o in parts])
    for k in far:
        S.append([
            link(Y.at[rank[k], ox[o]], RS.at[k - 2, o], x_peer)
            if sum_y[k][o]
            else link(Y.at[other[k], mx[o]], RS.at[k - 2, o], y_peer)
            for o in parts
        ])
    start = len(sent)
    ZR = [None, None] + [
        [link(Y.at[rank[k], mx[o]], RZ.at[kind, o], z_peer[k], start + kind * quarter + o) for o in parts] for k in far
    ]
    ZA = [[arrival(RZ.at[i, o], start + i * quarter + o) for o in parts] for i in both]
    ZR1 = [[link(Y.at[TG[1][o][i]], RZ1.at[o, i], z_peer[1]) for i in both] for o in parts]
    E = [
        [link(Y.at[me, ox[o]], RE.at[o, 0], x_peer), link(Y.at[me, mx[o]], RE.at[o, 1], x_peer)]
        if sum_y[0][o]
        else [link(Y.at[other[0], mx[o]], RE.at[o, 0], y_peer), None]
        for o in parts
    ]
    FX = [None if sum_y[0][o] else same(OUT.at[mx[o]], x_peer) for o in parts]
    FC = [same(OUT.at[mx[o]], core_peer) for o in parts]
    LC = [same(OUT.at[ox[o]], core_peer) for o in parts]

    for copy in route_loads:
        copy.wait()
    lane = lax.broadcasted_iota(jnp.int32, IDS.shape, 1)
    alive = lane < live[0]
    named = IDS[...]
    weight = jnp.sum(jnp.where((named == ex) & alive, GATES[...], 0.0), axis=0, keepdims=True)
    row = lax.broadcasted_iota(jnp.int32, M.shape[1:], 0)
    col = lax.broadcasted_iota(jnp.int32, M.shape[1:], 1)
    line = jnp.where(row == 0, weight, 0.0)
    for e in range(n_experts):
        count = jnp.sum(jnp.where((named == e) & alive, 1.0, 0.0))
        line = jnp.where((row == 1) & (col == e), count, line)
    M[me] = line

    for copy in own_loads:
        copy.wait()
    pl.semaphore_wait(barrier, len(peers))

    go(*metas)
    first_sends = [copy for o in parts for copy in (A0[o], ZS[3][o], ZS[2][o])]
    first_sends += [copy for o in parts if y_first[1][o] for copy in Z1[o]]

    def st(i):
        go(first_sends[i])

    h_tile = min(256, WG.shape[1])

    def a0(o):
        got(A0[o])
        go(B0[o], D0[0][o])
        if not y_first[1][o]:
            go(*Z1[o])

    def b0(o):
        got(B0[o])
        go(D0[1][o])

    def fz(o, i):
        got(Z1[o][i])
        go(F1[o][i], D1[o][i])

    def zg(k, o):
        got(ZG[k][o])
        go(*((GY[k][o], GX[k][o]) if y_first[k][o] else (GX[k][o], GY[k][o])), DZ[k][o])

    def gh(k, o):
        got((GX, GY)[y_first[k][o]][k][o])
        go(GH[k][o], DF[k][o])

    def f1(o, i):
        got(F1[o][i])
        go(D1[o][2 + i])

    def gb(k, o):
        got((GY, GX)[y_first[k][o]][k][o])
        go(DR[k][o][0])

    def gc(k, o):
        got(GH[k][o])
        go(DR[k][o][1])

    def whole(k):
        if k == 0:
            got(*D0[0], *D0[1])
        elif k == 1:
            got(*[copy for o in parts for copy in D1[o]])
        else:
            got(*DZ[k], *DF[k], *[copy for o in parts for copy in DR[k][o]])

    def tiles(tile, lo, hi):
        for t in range(lo, hi):
            tile(t)

    scales = {}

    def gate_up(k, lo, hi):
        if k not in scales:
            if not scales:
                got(*metas)
                weight_loads[0].wait()
                weight_loads[1].wait()
            columns = [jnp.transpose(M[member[k][j]])[:, 0:1] for j in range(n_y)]
            scales[k] = jnp.concatenate(columns, axis=0)

        def tile(t):
            cols = pl.ds(t * h_tile, h_tile)
            lhs = jnp.concatenate([G[pair[k], q].reshape(n_y * rows, width) for q in range(pieces)], axis=1)
            g = jnp.dot(lhs, WG[:, cols], preferred_element_type=F32)
            u = jnp.dot(lhs, WU[:, cols], preferred_element_type=F32)
            H[k, :, cols] = (g / (1.0 + jnp.exp(-g)) * u * scales[k]).astype(BF16)

        tiles(tile, lo, hi)

    downs, per = [], pieces // 4

    def down(k, lo, hi):
        if not downs:
            weight_loads[2].wait()
        downs.append(k)

        def tile(t):
            q = (co, c)[t // 2] * half + sides[t % 2]
            cols = pl.ds(pl.multiple_of(q * width, width), per * width)
            part = jnp.dot(H[k], WD[:, cols], preferred_element_type=F32).astype(BF16)
            for i in range(per):
                Y[pair[k], q + i] = part[:, i * width:(i + 1) * width].reshape(n_y, rows, width)

        tiles(tile, lo, hi)

    def add(r, q, value):
        Y[r, q] = (Y[r, q].astype(F32) + value.astype(F32)).astype(BF16)

    def r1(k, h):
        got(C[k][h])
        for j in range(n_y):
            def tile(i, carry):
                add(member[k][j], c * half + sides[h] + i, RC[k, j, sides[h] + i])
                return carry
            lax.fori_loop(0, quarter, tile, 0)
        for o in parts:
            if sum_y[k][o]:
                go(T[k][o][h])
            elif h == 0:
                go(*T[k][o])

    def r2(k, o):
        for i in both:
            got(T[k][o][i])
            add(*TG[k][o][i], RT[k, o, i])
            if k == 1:
                go(ZR1[o][i])
        if k > 1:
            go(S[k][o])

    def r3(k, o):
        got(S[k][o])
        add(rank[k], mx[o], RS[k - 2, o])
        go(ZR[k][o])

    def rz1(o):
        for i in both:
            got(ZR1[o][i])
            add(*TG[0][o][i], RZ1[o, i])
            if i == (0 if sum_y[0][o] else 1):
                go(E[o][0])

    def last(o):
        total = Y[me, mx[o]].astype(F32)
        if not sum_y[0][o]:
            got(E[o][0])
            total = total + RE[o, 0].astype(F32)
        got(ZA[0][o], ZA[1][o])
        total = (total + RZ[0, o].astype(F32) + RZ[1, o].astype(F32)).astype(BF16)
        if sum_y[0][o]:
            Y[me, mx[o]] = total
            go(E[o][1])
        else:
            OUT[mx[o]] = total
            go(FX[o], FC[o])

    def fin(o):
        if sum_y[0][o]:
            for i, q, copy in ((0, mx[o], FC[o]), (1, ox[o], LC[o])):
                got(E[o][i])
                OUT[q] = (Y[me, q].astype(F32) + RE[o, i].astype(F32)).astype(BF16)
                go(copy)
        else:
            got(FX[o])
            go(LC[o])

    def loads():
        count = M[0]
        for r in range(1, n_dp):
            count = count + M[r]
        LOADS[...] = count

    st(2)
    st(10)
    st(0)
    st(6)
    st(7)
    st(1)
    st(3)
    st(8)
    st(9)
    st(4)
    st(11)
    st(5)
    st(15)
    a0(0)
    st(14)
    a0(2)
    a0(1)
    a0(3)
    zg(3, 2)
    zg(3, 0)
    b0(3)
    zg(3, 3)
    b0(0)
    st(12)
    b0(1)
    zg(3, 1)
    b0(2)
    whole(0)
    gh(3, 0)
    gh(3, 2)
    gate_up(0, 0, 1)
    gh(3, 3)
    gb(3, 3)
    fz(3, 1)
    gb(3, 2)
    gh(3, 1)
    fz(0, 0)
    st(13)
    gate_up(0, 1, 3)
    gc(3, 2)
    fz(0, 1)
    zg(2, 2)
    zg(2, 0)
    gb(3, 0)
    gc(3, 3)
    fz(3, 0)
    gc(3, 0)
    gb(3, 1)
    gate_up(0, 3, 4)
    gc(3, 1)
    whole(3)
    zg(2, 3)
    gate_up(3, 0, 2)
    fz(2, 0)
    fz(1, 0)
    gate_up(3, 2, 3)
    gh(2, 0)
    f1(0, 0)
    fz(2, 1)
    fz(1, 1)
    zg(2, 1)
    gh(2, 2)
    gate_up(3, 3, 4)
    down(3, 0, 1)
    go(C[3][0])
    down(3, 1, 2)
    go(C[3][1])
    f1(0, 1)
    down(3, 2, 3)
    f1(1, 0)
    f1(2, 0)
    down(0, 0, 1)
    go(C[0][0])
    gh(2, 3)
    r1(3, 0)
    f1(3, 0)
    gb(2, 3)
    f1(1, 1)
    down(3, 3, 4)
    r1(3, 1)
    f1(3, 1)
    f1(2, 1)
    gh(2, 1)
    down(0, 1, 2)
    go(C[0][1])
    down(0, 2, 3)
    whole(1)
    gate_up(1, 0, 3)
    gb(2, 1)
    r2(3, 2)
    down(0, 3, 4)
    r2(3, 0)
    gate_up(1, 3, 4)
    gc(2, 2)
    gb(2, 2)
    r1(0, 1)
    r2(3, 1)
    r1(0, 0)
    down(1, 0, 1)
    go(C[1][0])
    down(1, 1, 2)
    go(C[1][1])
    down(1, 2, 3)
    gc(2, 3)
    gc(2, 0)
    gc(2, 1)
    r3(3, 2)
    r1(1, 0)
    r2(3, 3)
    gb(2, 0)
    r3(3, 0)
    down(1, 3, 4)
    whole(2)
    r1(1, 1)
    gate_up(2, 0, 4)
    r3(3, 1)
    down(2, 0, 1)
    go(C[2][0])
    down(2, 1, 2)
    go(C[2][1])
    r2(1, 2)
    down(2, 2, 3)
    r2(1, 0)
    r1(2, 0)
    r2(0, 2)
    down(2, 3, 4)
    r3(3, 3)
    r1(2, 1)
    r2(2, 2)
    r2(2, 0)
    r2(2, 1)
    r2(1, 3)
    r3(2, 2)
    r2(2, 3)
    r3(2, 0)
    rz1(2)
    r3(2, 1)
    r2(1, 1)
    r2(0, 3)
    rz1(3)
    r3(2, 3)
    r2(0, 1)
    r2(0, 0)
    rz1(0)
    loads()
    last(2)
    last(0)
    rz1(1)
    last(1)
    last(3)
    fin(1)
    fin(0)
    fin(2)
    fin(3)

    for o in parts:
        got(FC[o], LC[o])
    for copy in sent:
        copy.wait_send()


def collect(values, loads, out, totals, sem):
    pieces, _, width = values.shape
    copies = [
        pltpu.make_async_copy(values.at[q], out.at[:, pl.ds(q * width, width)], sem.at[q]) for q in range(pieces)
    ]
    for copy in copies:
        copy.start()
    row = lax.broadcasted_iota(jnp.int32, loads.shape, 0)
    col = lax.broadcasted_iota(jnp.int32, loads.shape, 1)
    for e in range(totals.shape[0]):
        totals[e] = jnp.sum(jnp.where((row == 1) & (col == e), loads[...], 0.0)).astype(jnp.int32)
    for copy in copies:
        copy.wait()


def planned(n_y, n_planes, tokens, expert_ids, gate_weights, live_counts, w_gate, w_up, w_down):
    n_experts = lax.axis_size("expert")
    rows, model = tokens.shape
    hidden = w_gate.shape[2]
    n_dp, pieces = n_y * n_planes, 16
    width, half, quarter = model // pieces, pieces // 2, pieces // 4
    hbm = pl.BlockSpec(memory_space=pl.ANY)
    smem = pl.BlockSpec(memory_space=pltpu.SMEM)
    vmem = pl.BlockSpec(memory_space=pltpu.VMEM)
    values, loads = pl.pallas_call(
        functools.partial(kernel, n_y, n_planes, n_experts),
        name="moe",
        out_shape=(pltpu.VMEM((pieces, rows, width), BF16), pltpu.VMEM((8, rows), F32)),
        in_specs=[hbm] * 3 + [smem] + [hbm] * 3,
        out_specs=(vmem, vmem),
        scratch_shapes=[
            pltpu.VMEM((n_dp, pieces, rows, width), BF16),
            pltpu.VMEM((n_dp, 8, rows), F32),
            pltpu.VMEM((2, rows), jnp.int32),
            pltpu.VMEM((2, rows), F32),
            pltpu.VMEM((model, hidden), BF16),
            pltpu.VMEM((model, hidden), BF16),
            pltpu.VMEM((hidden, model), BF16),
            pltpu.VMEM((n_planes, n_y * rows, hidden), BF16),
            pltpu.VMEM((n_dp, pieces, rows, width), BF16),
            pltpu.VMEM((n_planes, n_y, half, rows, width), BF16),
            pltpu.VMEM((n_planes, quarter, 2, rows, width), BF16),
            pltpu.VMEM((2, quarter, rows, width), BF16),
            pltpu.VMEM((quarter, 2, rows, width), BF16),
            pltpu.VMEM((quarter, 2, rows, width), BF16),
            pltpu.VMEM((2, quarter, rows, width), BF16),
            pltpu.SemaphoreType.DMA((224,)),
            pltpu.SemaphoreType.DMA((224,)),
            pltpu.SemaphoreType.DMA((64,)),
        ],
        compiler_params=pltpu.CompilerParams(
            collective_id=0, has_side_effects=True, vmem_limit_bytes=56 * 2**20
        ),
    )(tokens, expert_ids.T, gate_weights.T, live_counts, w_gate, w_up, w_down)
    return pl.pallas_call(
        collect,
        name="collect",
        out_shape=(jax.ShapeDtypeStruct((rows, model), BF16), jax.ShapeDtypeStruct((n_experts,), jnp.int32)),
        in_specs=[vmem, vmem],
        out_specs=(hbm, smem),
        scratch_shapes=[pltpu.SemaphoreType.DMA((pieces,))],
        compiler_params=pltpu.CompilerParams(vmem_limit_bytes=4 * 2**20),
    )(values, loads)


def solution(mesh):
    n_dp, n_experts = mesh.shape["dp"], mesh.shape["expert"]
    n_x = n_experts // 2
    n_y = n_x
    n_planes = n_dp // n_y
    body = general
    if n_y == 2 and n_planes == 4:
        body = functools.partial(planned, n_y, n_planes)
    placed = (
        P("dp", None),
        P("dp", None),
        P("dp", None),
        P("dp"),
        P("expert", None, "dp"),
        P("expert", None, "dp"),
        P("expert", "dp", None),
    )
    return jax.shard_map(
        body, mesh=mesh, in_specs=placed, out_specs=(P("dp", None), P()), check_vma=False
    )
```
